32 devices in a mesh: field: 2 (over x), expo: 8 (over z, y), sky: 2 (over core).
Axes of the slice: x: 2, y: 2, z: 4, core: 2. Of those that a mesh axis runs over, the one named last changes fastest.
Arguments:
- science: float32 [64, 64, 512], P(('field', 'expo'), 'sky'), parts along dimension 0, may hold values from -6 to 6
- inv_variance: float32 [64, 64, 512], P(('field', 'expo'), 'sky'), parts along dimension 0, may hold values from 0.25 to 4
- pixel_masks: int32 [64, 64, 512], P(('field', 'expo'), 'sky'), parts along dimension 0, may hold values 0 or 1
- point_spread: float32 [64, 5, 5], P(('field', 'expo')), parts along dimension 0, may hold values from 0.02 to 0.1
- tile_offset: int32 [8, 32], P(None, 'expo'), may hold values from 0 to 1
- column_shift: int32 [8, 32], P(None, 'expo'), may hold values from -128 to 128
- trail_kernel: float32 [8, 3, 3], P('expo'), may hold values from 0.1 to 1
Outputs:
- likelihood: float32 [16, 64, 512], P(('field', 'expo'), 'sky'), parts along dimension 0
The draws below stay inside these ranges and needn't reach their ends.
There are 2 independent parts, one for each index of `field`. The reference program is written for one: setup_inputs(seed, part) draws one part's arguments, and reference() takes and returns one part's arrays. A program takes and returns all parts, laid end to end along the dimension named above; an argument that names none is the same for every part. Nothing has to cross between parts.
All inputs are finite; a program needn't handle non-finite values. No bound on the sum of `pixel_masks` on one device may be relied on, other than what follows from the above.
Results may differ from the reference program's by a relative error of at most 0.0003.
Values sent between devices are 32-bit elements; how exact they have to be, the bound alone decides.
No kernel may reach another device: no remote copies, remote signals or barrier semaphores. Data moves between devices by JAX's collectives and lax.ppermute only.
A program may use at most 128 MiB of HBM per device.

```python
import math
import jax
import jax.numpy as jnp
from jax import lax

ROWS_DEV = 32
W = 512
MAX_SHIFT = 128
E = 32
V = 8
H = 64


def plant(values, key, least, high):
    place = [jax.random.randint(jax.random.fold_in(key, axis), (), 0, length) for axis, length in enumerate(values.shape)]
    widest = values.shape.index(max(values.shape))
    beside = place[:widest] + [(place[widest] + 1) % values.shape[widest]] + place[widest + 1:]
    return values.at[tuple(place)].set(least).at[tuple(beside)].set(high)


def block_scale(rng, shape, cuts, smallest, top_value):
    level, own = 1.0, jax.random.fold_in(rng, 6)
    for position, blocks in cuts:
        steps = jnp.exp(jax.random.uniform(jax.random.fold_in(own, position), (blocks,), jnp.float32, smallest / len(cuts), top_value / len(cuts)))
        level = level * jnp.repeat(steps, shape[position] // blocks).reshape([-1 if axis == position else 1 for axis in range(len(shape))])
    return level


def gaussian(rng, extent, deviation, reach, cuts=(), kind=jnp.bfloat16):
    drawn = deviation * jax.random.normal(rng, extent, jnp.float32)
    if cuts:
        drawn = drawn * block_scale(rng, extent, cuts, -0.22, 0.18)
    return jnp.clip(drawn, -reach, reach).astype(kind)


def setup_inputs(seed: int = 0, part: int = 0) -> dict:
    key_list = jax.random.split(jax.random.key(seed), 8)
    part_keys = jax.random.split(jax.random.fold_in(key_list[7], part), 8)
    science = gaussian(part_keys[0], (E, H, W), 1.0, 6.0, ((0, 8), (1, 2)), jnp.float32)
    inv_variance = jnp.clip(jnp.exp(math.log(4.0) - 2.7725887 * jax.random.uniform(part_keys[1], (E, H, W), jnp.float32) ** block_scale(part_keys[1], (E, H, W), ((0, 8), (1, 2)), -0.2, 0.2)), 0.25, 4.0)
    pixel_masks = plant((jax.random.randint(part_keys[2], (E, H, W), 0, 8) < 7).astype(jnp.int32), jax.random.fold_in(part_keys[2], 1), 0, 1)
    point_spread = jnp.clip(0.02 + 0.08 * jax.random.uniform(part_keys[3], (E, 5, 5), jnp.float32) ** block_scale(part_keys[3], (E, 5, 5), ((0, 8),), -0.2, 0.2), 0.02, 0.1)
    tile_offset = plant(jax.random.randint(key_list[4], (V, E), 0, 2), jax.random.fold_in(key_list[4], 1), 0, 1).astype(jnp.int32)
    column_shift = plant(jax.random.randint(key_list[5], (V, E), 0 - MAX_SHIFT, MAX_SHIFT + 1), jax.random.fold_in(key_list[5], 1), 0 - MAX_SHIFT, MAX_SHIFT).astype(jnp.int32)
    trail_kernel = jnp.clip(0.1 + 0.9 * jax.random.uniform(key_list[6], (V, 3, 3), jnp.float32) ** block_scale(key_list[6], (V, 3, 3), ((0, 8),), -0.2, 0.2), 0.1, 1.0)
    return {"science": science, "inv_variance": inv_variance, "pixel_masks": pixel_masks, "point_spread": point_spread, "tile_offset": tile_offset, "column_shift": column_shift, "trail_kernel": trail_kernel}


def filter_taps(padded, kernel, row_count, column_count):
    taps = kernel.shape[-1]
    running = jnp.zeros(padded.shape[:-2] + (row_count, column_count), jnp.float32)
    for row_tap in range(taps):
        for column_tap in range(taps):
            running = running + kernel[:, row_tap, column_tap, None, None] * padded[..., row_tap:row_tap + row_count, column_tap:column_tap + column_count]
    return running

def shift_columns(wide, column_shifts, column_count):
    margin = (wide.shape[-1] - column_count) // 2

    def single(single_image, pixel_shift):
        return lax.dynamic_slice_in_dim(single_image, (margin - pixel_shift).astype(jnp.int32), column_count, 2)
    return jax.vmap(single, in_axes=(1, 0), out_axes=1)(wide, column_shifts)

def reference(science, inv_variance, pixel_masks, point_spread, tile_offset, column_shift, trail_kernel):
    row_count = science.shape[1]
    column_count = science.shape[2]
    weighted = inv_variance * pixel_masks.astype(jnp.float32)
    signal = science * weighted
    psi_images = filter_taps(jnp.pad(signal, ((0, 0), (2, 2), (2, 2))), point_spread, row_count, column_count)
    phi_images = filter_taps(jnp.pad(weighted, ((0, 0), (2, 2), (2, 2))), point_spread * point_spread, row_count, column_count)
    filtered = jnp.stack([psi_images, phi_images])
    rolled = jnp.roll(filtered, -ROWS_DEV, axis=2)
    padding = ((0, 0), (0, 0), (0, 0), (MAX_SHIFT, MAX_SHIFT))
    own_wide = jnp.pad(filtered, padding)
    rolled_wide = jnp.pad(rolled, padding)

    def stack_velocity(inputs):
        offsets, column_shifts = inputs
        source_wide = jnp.where(offsets[None, :, None, None] == 1, rolled_wide, own_wide)
        return lax.optimization_barrier(jnp.sum(shift_columns(source_wide, column_shifts, column_count), axis=1))
    stacks = lax.map(stack_velocity, (tile_offset, column_shift))
    rimmed = jnp.pad(stacks, ((0, 0), (0, 0), (1, 1), (1, 1)))
    psi_trail = filter_taps(rimmed[:, 0], trail_kernel, row_count, column_count)
    phi_trail = filter_taps(rimmed[:, 1], trail_kernel * trail_kernel, row_count, column_count)
    return psi_trail / jnp.sqrt(phi_trail + 1.0)
```

```python
import functools

import jax
import jax.numpy as jnp
from jax import lax
from jax.experimental import pallas as pl
from jax.experimental.pallas import tpu as pltpu
from jax.sharding import PartitionSpec as P

MAX_SHIFT = 128
LANES = 128
SUB = 8


def lane_shifted(pieces, lane, offset):
    if offset == 0:
        return pieces
    count = len(pieces)
    rolled = [pltpu.roll(piece, (-offset) % LANES, 1) for piece in pieces]
    out = []
    for c in range(count):
        near = rolled[c]
        if offset > 0:
            far = rolled[c + 1] if c + 1 < count else jnp.zeros_like(near)
            out.append(jnp.where(lane < LANES - offset, near, far))
        else:
            far = rolled[c - 1] if c > 0 else jnp.zeros_like(near)
            out.append(jnp.where(lane >= -offset, near, far))
    return out


def filter_rows(load, taps, row_taps, chunks, lane):
    half = row_taps // 2
    columns = [[None] * chunks for _ in range(row_taps)]
    for c in range(chunks):
        rows = [load(a, c) for a in range(row_taps)]
        for b in range(row_taps):
            total = rows[0] * taps[0][b]
            for a in range(1, row_taps):
                total = total + rows[a] * taps[a][b]
            columns[b][c] = total
    result = columns[half]
    for b in range(row_taps):
        if b != half:
            moved = lane_shifted(columns[b], lane, b - half)
            result = [x + y for x, y in zip(result, moved)]
    return result


def stack_kernel(
    where_ref, offset_ref, shift_ref, spread_ref, own_ref, other_ref, *rest,
    exposures, rows, chunks, taps, targets,
):
    outs = rest[: len(targets)]
    image, wide, edge = rest[len(targets):]
    sky = where_ref[0]
    height = 2 * rows
    lane = lax.broadcasted_iota(jnp.int32, (SUB, LANES), 1)
    zero = jnp.zeros((SUB, LANES), jnp.float32)
    kinds = 2
    own_base = pl.multiple_of(SUB + rows * sky, SUB)
    other_base = pl.multiple_of(SUB + rows * (1 - sky), SUB)
    for k in range(kinds):
        for e in range(exposures):
            for c in range(chunks):
                image[k, e, c, 0:SUB, :] = zero
                image[k, e, c, SUB + height :, :] = zero
                at = slice(c * LANES, (c + 1) * LANES)
                image[k, e, c, pl.ds(own_base, rows), :] = own_ref[k, e, :, at]
                image[k, e, c, pl.ds(other_base, rows), :] = other_ref[k, e, :, at]
    blank = jnp.zeros((height, LANES), jnp.float32)
    for e in range(exposures):
        for k in range(kinds):
            wide[e, k, 0] = blank
            wide[e, k, chunks + 1] = blank
            wide[e, k, chunks + 2] = blank
        for t in range(2):
            for c in (0, chunks + 1, chunks + 2):
                edge[e, t, c] = zero

    half = taps // 2
    groups = height // SUB
    for e in range(exposures):
        for k in range(kinds):
            scale = [[spread_ref[e, a * taps + b] for b in range(taps)] for a in range(taps)]
            if k == 1:
                scale = [[x * x for x in line] for line in scale]
            for g in range(groups):
                def load(a, c):
                    return image[k, e, c, SUB + g * SUB + a - half : SUB + g * SUB + a - half + SUB, :]

                result = filter_rows(load, scale, taps, chunks, lane)
                for c in range(chunks):
                    wide[e, k, 1 + c, g * SUB : (g + 1) * SUB, :] = result[c]
    at_row = (rows - 1) * sky
    for e in range(exposures):
        for t in range(2):
            for k in range(kinds):
                for c in range(chunks):
                    edge[e, t, 1 + c, k : k + 1, :] = wide[e, k, 1 + c, pl.ds(rows * t + at_row, 1), :]

    per = outs[0].shape[0]
    for index in range(len(targets)):
        out = outs[index]
        first = where_ref[1 + index]
        for p in range(per):
            v = first * per + p
            totals = [None, None]
            edges = None
            for e in range(exposures):
                tile = lax.rem(sky + offset_ref[v, e], 2)
                start = MAX_SHIFT - shift_ref[v, e]
                skip = lax.div(start, LANES)
                turn = lax.rem(start, LANES)
                back = lax.rem(LANES - turn, LANES)
                keep = lane < LANES - turn
                base = pl.multiple_of(tile * rows, SUB)
                for k in range(kinds):
                    moved = [
                        [
                            pltpu.roll(wide[e, k, skip + c, pl.ds(pl.multiple_of(base + g * SUB, SUB), SUB), :], back, 1)
                            for g in range(rows // SUB)
                        ]
                        for c in range(chunks + 1)
                    ]
                    picked = [
                        [jnp.where(keep, moved[c][g], moved[c + 1][g]) for g in range(rows // SUB)]
                        for c in range(chunks)
                    ]
                    if totals[k] is None:
                        totals[k] = picked
                    else:
                        totals[k] = [[x + y for x, y in zip(p0, p1)] for p0, p1 in zip(totals[k], picked)]
                moved = [pltpu.roll(edge[e, 1 - tile, skip + c], back, 1) for c in range(chunks + 1)]
                picked = [jnp.where(keep, moved[c], moved[c + 1]) for c in range(chunks)]
                edges = picked if edges is None else [x + y for x, y in zip(edges, picked)]
            for k in range(kinds):
                for c in range(chunks):
                    for g in range(rows // SUB):
                        row = (k * chunks + c) * rows + g * SUB
                        out[p, row : row + SUB, :] = totals[k][c][g]
            for c in range(chunks):
                row = kinds * chunks * rows + kinds * c
                out[p, row : row + kinds, :] = edges[c][0:kinds, :]


def trail_kernel_body(where_ref, trail_ref, *rest, rows, chunks, taps):
    parts = rest[:-2]
    out, image = rest[-2:]
    sky = where_ref[0]
    lane = lax.broadcasted_iota(jnp.int32, (SUB, LANES), 1)
    zero = jnp.zeros((SUB, LANES), jnp.float32)
    half = taps // 2
    groups = rows // SUB
    for p in range(out.shape[0]):
        def total(row, count):
            value = parts[0][p, row : row + count, :]
            for part in parts[1:]:
                value = value + part[p, row : row + count, :]
            return value

        results = []
        edges = total(2 * chunks * rows, 2 * chunks)
        for k in range(2):
            for c in range(chunks):
                image[c, 0:SUB, :] = zero
                image[c, SUB + rows :, :] = zero
                for g in range(groups):
                    image[c, SUB + g * SUB : SUB + (g + 1) * SUB, :] = total((k * chunks + c) * rows + g * SUB, SUB)
                at = jnp.where(sky == 0, SUB + rows, SUB - 1)
                image[c, pl.ds(at, 1), :] = edges[2 * c + k : 2 * c + k + 1, :]
            scale = [[trail_ref[p, a * taps + b] for b in range(taps)] for a in range(taps)]
            if k == 1:
                scale = [[x * x for x in line] for line in scale]
            kind = []
            for g in range(groups):
                def load(a, c):
                    return image[c, SUB + g * SUB + a - half : SUB + g * SUB + a - half + SUB, :]

                kind.append(filter_rows(load, scale, taps, chunks, lane))
            results.append(kind)
        for g in range(groups):
            for c in range(chunks):
                value = results[0][g][c] / jnp.sqrt(results[1][g][c] + 1.0)
                out[p, g * SUB : (g + 1) * SUB, c * LANES : (c + 1) * LANES] = value


SMEM = pl.BlockSpec(memory_space=pltpu.SMEM)
VMEM = pl.BlockSpec(memory_space=pltpu.VMEM)


def shards(
    science, inv_variance, pixel_masks, point_spread, tile_offset, column_shift, trail_kernel
):
    exposures, rows, width = science.shape
    chunks = width // LANES
    taps = point_spread.shape[-1]
    trail_taps = trail_kernel.shape[-1]
    count = lax.axis_size("expo")
    per = tile_offset.shape[0] // count
    inner = 2 if count % 2 == 0 else 1
    outer = count // inner
    me = lax.axis_index("expo")
    sky = lax.axis_index("sky")
    my_outer, my_inner = me // inner, me % inner

    weighted = inv_variance * pixel_masks.astype(jnp.float32)
    own = jnp.stack([science * weighted, weighted])
    other = lax.ppermute(own, "sky", [(0, 1), (1, 0)])

    hops = [(d, i) for d in list(range(outer - 1, -1, -1)) for i in range(inner - 1, -1, -1)]
    targets = [((my_outer + d) % outer) * inner + (my_inner + i) % inner for d, i in hops]
    where = jnp.stack([sky.astype(jnp.int32)] + [t.astype(jnp.int32) for t in targets])
    length = 2 * chunks * rows + 2 * chunks
    part = jax.ShapeDtypeStruct((per, length, LANES), jnp.float32)
    offsets = lax.dynamic_slice_in_dim
    partials = pl.pallas_call(
        functools.partial(
            stack_kernel, exposures=exposures, rows=rows, chunks=chunks, taps=taps, targets=targets
        ),
        out_shape=[part] * len(hops),
        in_specs=[SMEM, SMEM, SMEM, SMEM, VMEM, VMEM],
        out_specs=[VMEM] * len(hops),
        scratch_shapes=[
            pltpu.VMEM((2, exposures, chunks, 2 * rows + 2 * SUB, LANES), jnp.float32),
            pltpu.VMEM((exposures, 2, chunks + 3, 2 * rows, LANES), jnp.float32),
            pltpu.VMEM((exposures, 2, chunks + 3, SUB, LANES), jnp.float32),
        ],
        compiler_params=pltpu.CompilerParams(vmem_limit_bytes=24 * 1024 * 1024),
        name="stack",
    )(where, tile_offset, column_shift, point_spread.reshape(exposures, taps * taps), own, other)

    parts = dict(zip(hops, partials))
    arrived = []
    for d in range(outer - 1, -1, -1):
        total = parts[(d, 0)]
        for i in range(1, inner):
            pairs = [
                (o * inner + j, o * inner + (j + i) % inner) for o in range(outer) for j in range(inner)
            ]
            total = total + lax.ppermute(parts[(d, i)], "expo", pairs)
        if d:
            pairs = [
                (o * inner + j, ((o + d) % outer) * inner + j) for o in range(outer) for j in range(inner)
            ]
            total = lax.ppermute(total, "expo", pairs)
        arrived.append(total)

    return pl.pallas_call(
        functools.partial(trail_kernel_body, rows=rows, chunks=chunks, taps=trail_taps),
        out_shape=jax.ShapeDtypeStruct((per, rows, width), jnp.float32),
        in_specs=[SMEM, SMEM] + [VMEM] * len(arrived),
        out_specs=VMEM,
        scratch_shapes=[pltpu.VMEM((chunks, rows + 2 * SUB, LANES), jnp.float32)],
        compiler_params=pltpu.CompilerParams(vmem_limit_bytes=8 * 1024 * 1024),
        name="trail",
    )(where[:1], trail_kernel.reshape(per, trail_taps * trail_taps), *arrived)


def solution(mesh):
    return jax.shard_map(
        shards,
        mesh=mesh,
        in_specs=(
            P(("field", "expo"), "sky", None),
            P(("field", "expo"), "sky", None),
            P(("field", "expo"), "sky", None),
            P(("field", "expo"), None, None),
            P(None, "expo"),
            P(None, "expo"),
            P("expo", None, None),
        ),
        out_specs=P(("field", "expo"), "sky", None),
        check_vma=False,
    )
```

```python
import functools

import jax
import jax.numpy as jnp
from jax import lax
from jax.experimental import pallas as pl
from jax.experimental.pallas import tpu as pltpu
from jax.sharding import PartitionSpec as P


MAX_SHIFT = 128
LANES = 128
SUB = 8


def lane_shifted(pieces, lane, offset):
    if offset == 0:
        return pieces
    count = len(pieces)
    rolled = [pltpu.roll(piece, (-offset) % LANES, 1) for piece in pieces]
    out = []
    for c in range(count):
        near = rolled[c]
        if offset > 0:
            far = rolled[c + 1] if c + 1 < count else jnp.zeros_like(near)
            out.append(jnp.where(lane < LANES - offset, near, far))
        else:
            far = rolled[c - 1] if c > 0 else jnp.zeros_like(near)
            out.append(jnp.where(lane >= -offset, near, far))
    return out


def filter_rows(load, taps, row_taps, chunks, lane):
    half = row_taps // 2
    columns = [[None] * chunks for _ in range(row_taps)]
    for c in range(chunks):
        rows = [load(a, c) for a in range(row_taps)]
        for b in range(row_taps):
            total = rows[0] * taps[0][b]
            for a in range(1, row_taps):
                total = total + rows[a] * taps[a][b]
            columns[b][c] = total
    result = columns[half]
    for b in range(row_taps):
        if b != half:
            moved = lane_shifted(columns[b], lane, b - half)
            result = [x + y for x, y in zip(result, moved)]
    return result


def filter_groups(image, wide, taps_of, first, count, exposures, chunks, taps, lane):
    half = taps // 2
    for e in range(exposures):
        for k in range(2):
            scale = taps_of(e, k)
            for g in range(count):
                row = pl.multiple_of((first + g) * SUB, SUB)

                def load(a, c):
                    return image[k, e, c, pl.ds(row + (SUB + a - half), SUB), :]

                result = filter_rows(load, scale, taps, chunks, lane)
                for c in range(chunks):
                    wide[e, k, 1 + c, pl.ds(row, SUB), :] = result[c]


def taps_in(spread_ref, taps):
    def taps_of(e, k):
        scale = [[spread_ref[a, e, b] for b in range(taps)] for a in range(taps)]
        return scale if k == 0 else [[x * x for x in line] for line in scale]

    return taps_of


def near_kernel(spread_ref, own_ref, image, wide, *, rows, chunks, taps):
    exposures = own_ref.shape[1]
    sky = lax.axis_index("sky")
    lane = lax.broadcasted_iota(jnp.int32, (SUB, LANES), 1)
    zero = jnp.zeros((SUB, LANES), jnp.float32)
    base = pl.multiple_of(SUB + rows * sky, SUB)
    for k in range(2):
        for e in range(exposures):
            for c in range(chunks):
                image[k, e, c, 0:SUB, :] = zero
                image[k, e, c, SUB + 2 * rows :, :] = zero
                image[k, e, c, pl.ds(base, rows), :] = own_ref[k, e, :, c * LANES : (c + 1) * LANES]
    inside = rows // SUB - 1
    first = (2 * (rows // SUB) - inside) * sky
    filter_groups(image, wide, taps_in(spread_ref, taps), first, inside, exposures, chunks, taps, lane)
    blank = jnp.zeros((2 * rows, LANES), jnp.float32)
    for e in range(exposures):
        for k in range(2):
            for c in (0, chunks + 1, chunks + 2):
                wide[e, k, c] = blank


def stack_velocity(out, p, v, wide, edge, offset_ref, shift_ref, sky, rows, chunks, lane):
    exposures = wide.shape[0]
    totals = [None, None]
    edges = None
    groups = rows // SUB
    for e in range(exposures):
        tile = lax.rem(sky + offset_ref[e, v], 2)
        start = MAX_SHIFT - shift_ref[e, v]
        skip = lax.div(start, LANES)
        turn = lax.rem(start, LANES)
        back = lax.rem(LANES - turn, LANES)
        keep = lane < LANES - turn
        base = pl.multiple_of(tile * rows, SUB)
        for k in range(2):
            moved = [
                [
                    pltpu.roll(wide[e, k, skip + c, pl.ds(pl.multiple_of(base + g * SUB, SUB), SUB), :], back, 1)
                    for g in range(groups)
                ]
                for c in range(chunks + 1)
            ]
            picked = [
                [jnp.where(keep, moved[c][g], moved[c + 1][g]) for g in range(groups)] for c in range(chunks)
            ]
            if totals[k] is None:
                totals[k] = picked
            else:
                totals[k] = [[x + y for x, y in zip(p0, p1)] for p0, p1 in zip(totals[k], picked)]
        moved = [pltpu.roll(edge[e, 1 - tile, skip + c], back, 1) for c in range(chunks + 1)]
        picked = [jnp.where(keep, moved[c], moved[c + 1]) for c in range(chunks)]
        edges = picked if edges is None else [x + y for x, y in zip(edges, picked)]
    for k in range(2):
        for c in range(chunks):
            for g in range(groups):
                row = (k * chunks + c) * rows + g * SUB
                out[p, row : row + SUB, :] = totals[k][c][g]
    for c in range(chunks):
        row = 2 * chunks * rows + 2 * c
        out[p, row : row + 2, :] = edges[c][0:2, :]


def stack_targets(outs, hops, inner, wide, edge, offset_ref, shift_ref, sky, rows, chunks, lane):
    me = lax.axis_index("expo")
    count = lax.axis_size("expo")
    for out, hop in zip(outs, hops):
        owner = target_of(me, hop, count, inner)
        for p in range(out.shape[0]):
            stack_velocity(
                out, p, owner * out.shape[0] + p, wide, edge, offset_ref, shift_ref, sky, rows, chunks, lane
            )


def target_of(index, hop, count, inner):
    far, near = hop
    outer = count // inner
    low = lax.rem(index, inner)
    high = lax.div(index, inner)
    if outer & (outer - 1) == 0:
        high = lax.bitwise_xor(high, jnp.int32(far))
    else:
        high = lax.rem(high + far, outer)
    return high * inner + lax.rem(low + near, inner)


def owner_index(index, hop, count, inner):
    far, near = hop
    outer = count // inner
    high, low = divmod(index, inner)
    high = high ^ far if outer & (outer - 1) == 0 else (high + far) % outer
    return high * inner + (low + near) % inner


def far_kernel(
    spread_ref, offset_ref, shift_ref, other_ref, image_in, wide_in, image, wide, edge, *outs,
    hops, inner, rows, chunks, taps,
):
    exposures = other_ref.shape[1]
    sky = lax.axis_index("sky")
    lane = lax.broadcasted_iota(jnp.int32, (SUB, LANES), 1)
    zero = jnp.zeros((SUB, LANES), jnp.float32)
    base = pl.multiple_of(SUB + rows * (1 - sky), SUB)
    for k in range(2):
        for e in range(exposures):
            for c in range(chunks):
                image[k, e, c, pl.ds(base, rows), :] = other_ref[k, e, :, c * LANES : (c + 1) * LANES]
    inside = rows // SUB - 1
    filter_groups(
        image, wide, taps_in(spread_ref, taps), inside * (1 - sky), 2 * (rows // SUB) - inside,
        exposures, chunks, taps, lane,
    )
    at_row = (rows - 1) * sky
    for e in range(exposures):
        for t in range(2):
            for c in (0, chunks + 1, chunks + 2):
                edge[e, t, c] = zero
            for k in range(2):
                for c in range(chunks):
                    edge[e, t, 1 + c, k : k + 1, :] = wide[e, k, 1 + c, pl.ds(rows * t + at_row, 1), :]
    stack_targets(outs, hops, inner, wide, edge, offset_ref, shift_ref, sky, rows, chunks, lane)


def rest_kernel(offset_ref, shift_ref, wide, edge, *outs, hops, inner, rows, chunks):
    sky = lax.axis_index("sky")
    lane = lax.broadcasted_iota(jnp.int32, (SUB, LANES), 1)
    stack_targets(outs, hops, inner, wide, edge, offset_ref, shift_ref, sky, rows, chunks, lane)


def trail_kernel_body(trail_ref, *rest, rows, chunks, taps):
    parts = rest[:-2]
    out, image = rest[-2:]
    sky = lax.axis_index("sky")
    lane = lax.broadcasted_iota(jnp.int32, (SUB, LANES), 1)
    zero = jnp.zeros((SUB, LANES), jnp.float32)
    half = taps // 2
    groups = rows // SUB
    for p in range(out.shape[0]):
        def total(row, count):
            value = parts[0][p, row : row + count, :]
            for part in parts[1:]:
                value = value + part[p, row : row + count, :]
            return value

        results = []
        edges = total(2 * chunks * rows, 2 * chunks)
        for k in range(2):
            for c in range(chunks):
                image[c, 0:SUB, :] = zero
                image[c, SUB + rows :, :] = zero
                for g in range(groups):
                    image[c, SUB + g * SUB : SUB + (g + 1) * SUB, :] = total((k * chunks + c) * rows + g * SUB, SUB)
                at = jnp.where(sky == 0, SUB + rows, SUB - 1)
                image[c, pl.ds(at, 1), :] = edges[2 * c + k : 2 * c + k + 1, :]
            scale = [[trail_ref[a, p, b] for b in range(taps)] for a in range(taps)]
            if k == 1:
                scale = [[x * x for x in line] for line in scale]
            kind = []
            for g in range(groups):
                def load(a, c):
                    return image[c, SUB + g * SUB + a - half : SUB + g * SUB + a - half + SUB, :]

                kind.append(filter_rows(load, scale, taps, chunks, lane))
            results.append(kind)
        for g in range(groups):
            for c in range(chunks):
                value = results[0][g][c] / jnp.sqrt(results[1][g][c] + 1.0)
                out[p, g * SUB : (g + 1) * SUB, c * LANES : (c + 1) * LANES] = value


SMEM = pl.BlockSpec(memory_space=pltpu.SMEM)
VMEM = pl.BlockSpec(memory_space=pltpu.VMEM)


def call(body, outputs, inputs, scratch=(), aliases={}, megabytes=8):
    return pl.pallas_call(
        body,
        out_shape=[jax.ShapeDtypeStruct(shape, jnp.float32) for shape in outputs],
        in_specs=[spec for spec, _ in inputs],
        out_specs=[VMEM] * len(outputs),
        scratch_shapes=scratch,
        input_output_aliases=aliases,
        compiler_params=pltpu.CompilerParams(vmem_limit_bytes=megabytes * 1024 * 1024),
    )(*[value for _, value in inputs])


def steps(
    science, inv_variance, pixel_masks, point_spread, tile_offset, column_shift, trail_kernel
):
    exposures, rows, width = science.shape
    chunks = width // LANES
    taps = point_spread.shape[-1]
    trail_taps = trail_kernel.shape[-1]
    count = lax.axis_size("expo")
    per = tile_offset.shape[0] // count
    inner = 2 if count % 2 == 0 else 1
    outer = count // inner

    weighted = inv_variance * pixel_masks.astype(jnp.float32)
    own = jnp.stack([science * weighted, weighted])
    other = lax.ppermute(own, "sky", [(0, 1), (1, 0)])

    spread = (SMEM, jnp.transpose(point_spread, (1, 0, 2)))
    offsets = (SMEM, tile_offset.T)
    shifts = (SMEM, column_shift.T)
    image_shape = (2, exposures, chunks, 2 * rows + 2 * SUB, LANES)
    wide_shape = (exposures, 2, chunks + 3, 2 * rows, LANES)
    edge_shape = (exposures, 2, chunks + 3, SUB, LANES)
    part = (per, 2 * chunks * rows + 2 * chunks, LANES)

    image, wide = call(
        functools.partial(near_kernel, rows=rows, chunks=chunks, taps=taps),
        [image_shape, wide_shape], [spread, (VMEM, own)],
    )
    far_order = far_first(outer)
    sends = [(d, i) for d in far_order for i in range(1, inner)]
    keeps = [(d, 0) for d in far_order]
    early = sends[:2] if inner > 1 else keeps[:1]
    late = [hop for hop in keeps + sends if hop not in early]
    late = sorted(late, key=lambda hop: far_order.index(hop[0]))
    results = call(
        functools.partial(far_kernel, hops=early, inner=inner, rows=rows, chunks=chunks, taps=taps),
        [image_shape, wide_shape, edge_shape] + [part] * len(early),
        [spread, offsets, shifts, (VMEM, other), (VMEM, image), (VMEM, wide)],
        aliases={4: 0, 5: 1},
    )
    wide, edge = results[1:3]
    parts = dict(zip(early, results[3:]))
    results = call(
        functools.partial(rest_kernel, hops=late, inner=inner, rows=rows, chunks=chunks),
        [part] * len(late), [offsets, shifts, (VMEM, wide), (VMEM, edge)],
    )
    parts.update(zip(late, results))

    def hop_pairs(hop):
        return [(i, int(owner_index(i, hop, count, inner))) for i in range(count)]

    arrived = []
    for d in far_order:
        total = parts[(d, 0)]
        for i in range(1, inner):
            moved = lax.ppermute(parts[(d, i)], "expo", hop_pairs((0, i)))
            total = total + moved
        if d:
            total = lax.ppermute(total, "expo", hop_pairs((d, 0)))
        arrived.append(total)

    return call(
        functools.partial(trail_kernel_body, rows=rows, chunks=chunks, taps=trail_taps),
        [(per, rows, width)],
        [(SMEM, jnp.transpose(trail_kernel, (1, 0, 2)))] + [(VMEM, value) for value in arrived],
        scratch=[pltpu.VMEM((chunks, rows + 2 * SUB, LANES), jnp.float32)],
    )[0]


def far_first(outer):
    return sorted(range(outer), key=lambda d: (2 * d < outer, d if 2 * d >= outer else -d))


def solution(mesh):
    return jax.shard_map(
        steps,
        mesh=mesh,
        in_specs=(
            P(("field", "expo"), "sky", None),
            P(("field", "expo"), "sky", None),
            P(("field", "expo"), "sky", None),
            P(("field", "expo"), None, None),
            P(None, "expo"),
            P(None, "expo"),
            P("expo", None, None),
        ),
        out_specs=P(("field", "expo"), "sky", None),
        check_vma=False,
    )
```

```python
import functools

import jax
import jax.numpy as jnp
from jax import lax
from jax.experimental import pallas as pl
from jax.experimental.pallas import tpu as pltpu
from jax.sharding import PartitionSpec as P


MAX_SHIFT = 128
LANES = 128
SUB = 8


def lane_shifted(pieces, lane, offset):
    if offset == 0:
        return pieces
    count = len(pieces)
    rolled = [pltpu.roll(piece, (-offset) % LANES, 1) for piece in pieces]
    out = []
    for c in range(count):
        near = rolled[c]
        if offset > 0:
            far = rolled[c + 1] if c + 1 < count else jnp.zeros_like(near)
            out.append(jnp.where(lane < LANES - offset, near, far))
        else:
            far = rolled[c - 1] if c > 0 else jnp.zeros_like(near)
            out.append(jnp.where(lane >= -offset, near, far))
    return out


def filter_rows(load, taps, row_taps, chunks, lane):
    half = row_taps // 2
    columns = [[None] * chunks for _ in range(row_taps)]
    for c in range(chunks):
        rows = [load(a, c) for a in range(row_taps)]
        for b in range(row_taps):
            total = rows[0] * taps[0][b]
            for a in range(1, row_taps):
                total = total + rows[a] * taps[a][b]
            columns[b][c] = total
    result = columns[half]
    for b in range(row_taps):
        if b != half:
            moved = lane_shifted(columns[b], lane, b - half)
            result = [x + y for x, y in zip(result, moved)]
    return result


def filter_groups(image, wide, taps_of, first, count, exposures, chunks, taps, lane):
    half = taps // 2
    for e in range(exposures):
        for k in range(2):
            scale = taps_of(e, k)
            for g in range(count):
                row = pl.multiple_of((first + g) * SUB, SUB)

                def load(a, c):
                    return image[k, e, c, pl.ds(row + (SUB + a - half), SUB), :]

                result = filter_rows(load, scale, taps, chunks, lane)
                for c in range(chunks):
                    wide[e, k, 1 + c, pl.ds(row, SUB), :] = result[c]


def taps_in(spread_ref, taps):
    def taps_of(e, k):
        scale = [[spread_ref[a, e, b] for b in range(taps)] for a in range(taps)]
        return scale if k == 0 else [[x * x for x in line] for line in scale]

    return taps_of


def near_kernel(spread_ref, own_ref, image, wide, *, rows, chunks, taps):
    exposures = own_ref.shape[1]
    sky = lax.axis_index("sky")
    lane = lax.broadcasted_iota(jnp.int32, (SUB, LANES), 1)
    zero = jnp.zeros((SUB, LANES), jnp.float32)
    base = pl.multiple_of(SUB + rows * sky, SUB)
    for k in range(2):
        for e in range(exposures):
            for c in range(chunks):
                image[k, e, c, 0:SUB, :] = zero
                image[k, e, c, SUB + 2 * rows :, :] = zero
                image[k, e, c, pl.ds(base, rows), :] = own_ref[k, e, :, c * LANES : (c + 1) * LANES]
    inside = rows // SUB - 1
    first = (2 * (rows // SUB) - inside) * sky
    filter_groups(image, wide, taps_in(spread_ref, taps), first, inside, exposures, chunks, taps, lane)
    blank = jnp.zeros((2 * rows, LANES), jnp.float32)
    for e in range(exposures):
        for k in range(2):
            for c in (0, chunks + 1, chunks + 2):
                wide[e, k, c] = blank


def stack_velocity(out, p, v, wide, edge, offset_ref, shift_ref, sky, rows, chunks, lane):
    exposures = wide.shape[0]
    totals = [None, None]
    edges = None
    groups = rows // SUB
    for e in range(exposures):
        tile = lax.rem(sky + offset_ref[e, v], 2)
        start = MAX_SHIFT - shift_ref[e, v]
        skip = lax.div(start, LANES)
        turn = lax.rem(start, LANES)
        back = lax.rem(LANES - turn, LANES)
        keep = lane < LANES - turn
        base = pl.multiple_of(tile * rows, SUB)
        for k in range(2):
            moved = [
                [
                    pltpu.roll(wide[e, k, skip + c, pl.ds(pl.multiple_of(base + g * SUB, SUB), SUB), :], back, 1)
                    for g in range(groups)
                ]
                for c in range(chunks + 1)
            ]
            picked = [
                [jnp.where(keep, moved[c][g], moved[c + 1][g]) for g in range(groups)] for c in range(chunks)
            ]
            if totals[k] is None:
                totals[k] = picked
            else:
                totals[k] = [[x + y for x, y in zip(p0, p1)] for p0, p1 in zip(totals[k], picked)]
        moved = [pltpu.roll(edge[e, 1 - tile, skip + c], back, 1) for c in range(chunks + 1)]
        picked = [jnp.where(keep, moved[c], moved[c + 1]) for c in range(chunks)]
        edges = picked if edges is None else [x + y for x, y in zip(edges, picked)]
    for k in range(2):
        for c in range(chunks):
            for g in range(groups):
                row = (k * chunks + c) * rows + g * SUB
                out[p, row : row + SUB, :] = totals[k][c][g]
    for c in range(chunks):
        row = 2 * chunks * rows + 2 * c
        out[p, row : row + 2, :] = edges[c][0:2, :]


def stack_targets(outs, hops, wide, edge, offset_ref, shift_ref, sky, rows, chunks, lane):
    me = lax.axis_index("expo")
    for out, hop in zip(outs, hops):
        owner = jnp.bitwise_xor(me, jnp.where(sky == 0, hop, turned(hop)))
        for p in range(out.shape[0]):
            stack_velocity(
                out, p, owner * out.shape[0] + p, wide, edge, offset_ref, shift_ref, sky, rows, chunks, lane
            )


def turned(hop):
    return (hop & ~3) | ((hop & 1) << 1) | ((hop >> 1) & 1)


def far_kernel(
    spread_ref, offset_ref, shift_ref, other_ref, image_in, wide_in, image, wide, edge, *outs,
    hops, rows, chunks, taps,
):
    exposures = other_ref.shape[1]
    sky = lax.axis_index("sky")
    lane = lax.broadcasted_iota(jnp.int32, (SUB, LANES), 1)
    zero = jnp.zeros((SUB, LANES), jnp.float32)
    base = pl.multiple_of(SUB + rows * (1 - sky), SUB)
    for k in range(2):
        for e in range(exposures):
            for c in range(chunks):
                image[k, e, c, pl.ds(base, rows), :] = other_ref[k, e, :, c * LANES : (c + 1) * LANES]
    inside = rows // SUB - 1
    filter_groups(
        image, wide, taps_in(spread_ref, taps), inside * (1 - sky), 2 * (rows // SUB) - inside,
        exposures, chunks, taps, lane,
    )
    at_row = (rows - 1) * sky
    for e in range(exposures):
        for t in range(2):
            for c in (0, chunks + 1, chunks + 2):
                edge[e, t, c] = zero
            for k in range(2):
                for c in range(chunks):
                    edge[e, t, 1 + c, k : k + 1, :] = wide[e, k, 1 + c, pl.ds(rows * t + at_row, 1), :]
    stack_targets(outs, hops, wide, edge, offset_ref, shift_ref, sky, rows, chunks, lane)


def rest_kernel(offset_ref, shift_ref, wide, edge, *outs, hops, rows, chunks):
    sky = lax.axis_index("sky")
    lane = lax.broadcasted_iota(jnp.int32, (SUB, LANES), 1)
    stack_targets(outs, hops, wide, edge, offset_ref, shift_ref, sky, rows, chunks, lane)


def trail_kernel_body(trail_ref, *rest, rows, chunks, taps):
    parts = rest[:-2]
    out, image = rest[-2:]
    sky = lax.axis_index("sky")
    lane = lax.broadcasted_iota(jnp.int32, (SUB, LANES), 1)
    zero = jnp.zeros((SUB, LANES), jnp.float32)
    half = taps // 2
    groups = rows // SUB
    for p in range(out.shape[0]):
        def total(row, count):
            value = parts[0][p, row : row + count, :]
            for part in parts[1:]:
                value = value + part[p, row : row + count, :]
            return value

        results = []
        edges = total(2 * chunks * rows, 2 * chunks)
        for k in range(2):
            for c in range(chunks):
                image[c, 0:SUB, :] = zero
                image[c, SUB + rows :, :] = zero
                for g in range(groups):
                    image[c, SUB + g * SUB : SUB + (g + 1) * SUB, :] = total((k * chunks + c) * rows + g * SUB, SUB)
                at = jnp.where(sky == 0, SUB + rows, SUB - 1)
                image[c, pl.ds(at, 1), :] = edges[2 * c + k : 2 * c + k + 1, :]
            scale = [[trail_ref[a, p, b] for b in range(taps)] for a in range(taps)]
            if k == 1:
                scale = [[x * x for x in line] for line in scale]
            kind = []
            for g in range(groups):
                def load(a, c):
                    return image[c, SUB + g * SUB + a - half : SUB + g * SUB + a - half + SUB, :]

                kind.append(filter_rows(load, scale, taps, chunks, lane))
            results.append(kind)
        for g in range(groups):
            for c in range(chunks):
                value = results[0][g][c] / jnp.sqrt(results[1][g][c] + 1.0)
                out[p, g * SUB : (g + 1) * SUB, c * LANES : (c + 1) * LANES] = value


SMEM = pl.BlockSpec(memory_space=pltpu.SMEM)
VMEM = pl.BlockSpec(memory_space=pltpu.VMEM)


def call(body, outputs, inputs, scratch=(), aliases={}, megabytes=8):
    return pl.pallas_call(
        body,
        out_shape=[jax.ShapeDtypeStruct(shape, jnp.float32) for shape in outputs],
        in_specs=[spec for spec, _ in inputs],
        out_specs=[VMEM] * len(outputs),
        scratch_shapes=scratch,
        input_output_aliases=aliases,
        compiler_params=pltpu.CompilerParams(vmem_limit_bytes=megabytes * 1024 * 1024),
    )(*[value for _, value in inputs])


def steps(
    science, inv_variance, pixel_masks, point_spread, tile_offset, column_shift, trail_kernel
):
    exposures, rows, width = science.shape
    chunks = width // LANES
    taps = point_spread.shape[-1]
    trail_taps = trail_kernel.shape[-1]
    count = lax.axis_size("expo")
    per = tile_offset.shape[0] // count

    weighted = inv_variance * pixel_masks.astype(jnp.float32)
    own = jnp.stack([science * weighted, weighted])
    other = lax.ppermute(own, "sky", [(0, 1), (1, 0)])

    spread = (SMEM, jnp.transpose(point_spread, (1, 0, 2)))
    offsets = (SMEM, tile_offset.T)
    shifts = (SMEM, column_shift.T)
    image_shape = (2, exposures, chunks, 2 * rows + 2 * SUB, LANES)
    wide_shape = (exposures, 2, chunks + 3, 2 * rows, LANES)
    edge_shape = (exposures, 2, chunks + 3, SUB, LANES)
    part = (per, 2 * chunks * rows + 2 * chunks, LANES)

    image, wide = call(
        functools.partial(near_kernel, rows=rows, chunks=chunks, taps=taps),
        [image_shape, wide_shape], [spread, (VMEM, own)],
    )
    early, late = sending_order(count)
    results = call(
        functools.partial(far_kernel, hops=early, rows=rows, chunks=chunks, taps=taps),
        [image_shape, wide_shape, edge_shape] + [part] * len(early),
        [spread, offsets, shifts, (VMEM, other), (VMEM, image), (VMEM, wide)],
        aliases={4: 0, 5: 1},
    )
    wide, edge = results[1:3]
    parts = dict(zip(early, results[3:]))
    results = call(
        functools.partial(rest_kernel, hops=late, rows=rows, chunks=chunks),
        [part] * len(late), [offsets, shifts, (VMEM, wide), (VMEM, edge)],
    )
    parts.update(zip(late, results))

    bit = 1
    while bit < count:
        pairs = [
            (2 * i + core, 2 * (i ^ (turned(bit) if core else bit)) + core)
            for i in range(count) for core in range(2)
        ]
        for hop in range(count - bit, 0, -2 * bit):
            moved = lax.ppermute(parts[hop], ("expo", "sky"), pairs)
            parts[hop - bit] = parts[hop - bit] + moved
        bit *= 2
    total = parts[0]

    return call(
        functools.partial(trail_kernel_body, rows=rows, chunks=chunks, taps=trail_taps),
        [(per, rows, width)],
        [(SMEM, jnp.transpose(trail_kernel, (1, 0, 2)))] + [(VMEM, total)],
        scratch=[pltpu.VMEM((chunks, rows + 2 * SUB, LANES), jnp.float32)],
    )[0]


def sending_order(count):
    hops = list(range(count - 1, 0, -2)) + list(range(count - 2, -1, -2))
    return hops[:2], hops[2:]


def solution(mesh):
    return jax.shard_map(
        steps,
        mesh=mesh,
        in_specs=(
            P(("field", "expo"), "sky", None),
            P(("field", "expo"), "sky", None),
            P(("field", "expo"), "sky", None),
            P(("field", "expo"), None, None),
            P(None, "expo"),
            P(None, "expo"),
            P("expo", None, None),
        ),
        out_specs=P(("field", "expo"), "sky", None),
        check_vma=False,
    )
```

```python
import functools

import jax
import jax.numpy as jnp
from jax import lax
from jax.experimental import pallas as pl
from jax.experimental.pallas import tpu as pltpu
from jax.sharding import PartitionSpec as P


MAX_SHIFT = 128
LANES = 128
SUB = 8


def lane_shifted(pieces, lane, offset):
    if offset == 0:
        return pieces
    count = len(pieces)
    rolled = [pltpu.roll(piece, (-offset) % LANES, 1) for piece in pieces]
    out = []
    for c in range(count):
        near = rolled[c]
        if offset > 0:
            far = rolled[c + 1] if c + 1 < count else jnp.zeros_like(near)
            out.append(jnp.where(lane < LANES - offset, near, far))
        else:
            far = rolled[c - 1] if c > 0 else jnp.zeros_like(near)
            out.append(jnp.where(lane >= -offset, near, far))
    return out


def filter_rows(load, taps, row_taps, chunks, lane):
    half = row_taps // 2
    columns = [[None] * chunks for _ in range(row_taps)]
    for c in range(chunks):
        rows = [load(a, c) for a in range(row_taps)]
        for b in range(row_taps):
            total = rows[0] * taps[0][b]
            for a in range(1, row_taps):
                total = total + rows[a] * taps[a][b]
            columns[b][c] = total
    result = columns[half]
    for b in range(row_taps):
        if b != half:
            moved = lane_shifted(columns[b], lane, b - half)
            result = [x + y for x, y in zip(result, moved)]
    return result


def filter_groups(image, wide, taps_of, first, count, exposures, chunks, taps, lane):
    half = taps // 2
    for e in range(exposures):
        for k in range(2):
            scale = taps_of(e, k)
            for g in range(count):
                row = pl.multiple_of((first + g) * SUB, SUB)

                def load(a, c):
                    return image[k, e, c, pl.ds(row + (SUB + a - half), SUB), :]

                result = filter_rows(load, scale, taps, chunks, lane)
                for c in range(chunks):
                    wide[e, k, 1 + c, pl.ds(row, SUB), :] = result[c]


def taps_in(spread_ref, taps):
    def taps_of(e, k):
        scale = [[spread_ref[a, e, b] for b in range(taps)] for a in range(taps)]
        return scale if k == 0 else [[x * x for x in line] for line in scale]

    return taps_of


def vectors_in(load, taps):
    return lambda e, k: [[load(e, k, a * taps + b) for b in range(taps)] for a in range(taps)]


def near_kernel(spread_ref, own_ref, image, wide, spread_out, *, rows, chunks, taps):
    exposures = own_ref.shape[1]
    sky = lax.axis_index("sky")
    lane = lax.broadcasted_iota(jnp.int32, (SUB, LANES), 1)
    zero = jnp.zeros((SUB, LANES), jnp.float32)
    base = pl.multiple_of(SUB + rows * sky, SUB)
    for k in range(2):
        for e in range(exposures):
            for c in range(chunks):
                image[k, e, c, 0:SUB, :] = zero
                image[k, e, c, SUB + 2 * rows :, :] = zero
                image[k, e, c, pl.ds(base, rows), :] = own_ref[k, e, :, c * LANES : (c + 1) * LANES]
    inside = rows // SUB - 1
    first = (2 * (rows // SUB) - inside) * sky
    scalars = taps_in(spread_ref, taps)

    def taps_of(e, k):
        scale = [[zero + x for x in line] for line in scalars(e, k)]
        for a in range(taps):
            for b in range(taps):
                spread_out[e, k, a * taps + b] = scale[a][b]
        return scale

    filter_groups(image, wide, taps_of, first, inside, exposures, chunks, taps, lane)
    blank = jnp.zeros((2 * rows, LANES), jnp.float32)
    for e in range(exposures):
        for k in range(2):
            for c in (0, chunks + 1, chunks + 2):
                wide[e, k, c] = blank


def stack_velocity(out, p, v, wide, edge, offset_ref, shift_ref, sky, rows, chunks, lane):
    exposures = wide.shape[0]
    totals = [None, None]
    edges = None
    groups = rows // SUB
    for e in range(exposures):
        tile = lax.rem(sky + offset_ref[e, v], 2)
        start = MAX_SHIFT - shift_ref[e, v]
        skip = lax.div(start, LANES)
        turn = lax.rem(start, LANES)
        back = lax.rem(LANES - turn, LANES)
        keep = lane < LANES - turn
        base = pl.multiple_of(tile * rows, SUB)
        for k in range(2):
            moved = [
                [
                    pltpu.roll(wide[e, k, skip + c, pl.ds(pl.multiple_of(base + g * SUB, SUB), SUB), :], back, 1)
                    for g in range(groups)
                ]
                for c in range(chunks + 1)
            ]
            picked = [
                [jnp.where(keep, moved[c][g], moved[c + 1][g]) for g in range(groups)] for c in range(chunks)
            ]
            if totals[k] is None:
                totals[k] = picked
            else:
                totals[k] = [[x + y for x, y in zip(p0, p1)] for p0, p1 in zip(totals[k], picked)]
        moved = [pltpu.roll(edge[e, 1 - tile, skip + c], back, 1) for c in range(chunks + 1)]
        picked = [jnp.where(keep, moved[c], moved[c + 1]) for c in range(chunks)]
        edges = picked if edges is None else [x + y for x, y in zip(edges, picked)]
    for k in range(2):
        for c in range(chunks):
            for g in range(groups):
                row = (k * chunks + c) * rows + g * SUB
                out[p, row : row + SUB, :] = totals[k][c][g]
    for c in range(chunks):
        row = 2 * chunks * rows + 2 * c
        out[p, row : row + 2, :] = edges[c][0:2, :]


def stack_targets(outs, hops, wide, edge, offset_ref, shift_ref, sky, rows, chunks, lane):
    me = lax.axis_index("expo")
    for out, hop in zip(outs, hops):
        owner = jnp.bitwise_xor(me, jnp.where(sky == 0, hop, turned(hop)))
        for p in range(out.shape[0]):
            stack_velocity(
                out, p, owner * out.shape[0] + p, wide, edge, offset_ref, shift_ref, sky, rows, chunks, lane
            )


def turned(hop):
    return (hop & ~3) | ((hop & 1) << 1) | ((hop >> 1) & 1)


def far_kernel(
    spread_ref, offset_from, shift_from, other_ref, image_in, wide_in, image, wide, edge, *rest,
    hops, rows, chunks, taps,
):
    outs = rest[: len(hops)]
    offset_ref, shift_ref, offset_sem, shift_sem = rest[len(hops):]
    offset_copy = pltpu.make_async_copy(offset_from, offset_ref, offset_sem)
    shift_copy = pltpu.make_async_copy(shift_from, shift_ref, shift_sem)
    offset_copy.start()
    shift_copy.start()
    exposures = other_ref.shape[1]
    sky = lax.axis_index("sky")
    lane = lax.broadcasted_iota(jnp.int32, (SUB, LANES), 1)
    zero = jnp.zeros((SUB, LANES), jnp.float32)
    base = pl.multiple_of(SUB + rows * (1 - sky), SUB)
    for k in range(2):
        for e in range(exposures):
            for c in range(chunks):
                image[k, e, c, pl.ds(base, rows), :] = other_ref[k, e, :, c * LANES : (c + 1) * LANES]
    inside = rows // SUB - 1
    filter_groups(
        image, wide, vectors_in(lambda e, k, i: spread_ref[e, k, i], taps), inside * (1 - sky),
        2 * (rows // SUB) - inside, exposures, chunks, taps, lane,
    )
    at_row = (rows - 1) * sky
    for e in range(exposures):
        for t in range(2):
            for c in (0, chunks + 1, chunks + 2):
                edge[e, t, c] = zero
            for k in range(2):
                for c in range(chunks):
                    edge[e, t, 1 + c, k : k + 1, :] = wide[e, k, 1 + c, pl.ds(rows * t + at_row, 1), :]
    offset_copy.wait()
    shift_copy.wait()
    stack_targets(outs, hops, wide, edge, offset_ref, shift_ref, sky, rows, chunks, lane)


def rest_kernel(offset_ref, shift_ref, wide, edge, *outs, hops, rows, chunks):
    sky = lax.axis_index("sky")
    lane = lax.broadcasted_iota(jnp.int32, (SUB, LANES), 1)
    stack_targets(outs, hops, wide, edge, offset_ref, shift_ref, sky, rows, chunks, lane)


def last_kernel(offset_ref, shift_ref, trail_ref, wide, edge, trail_out, *outs, hops, rows, chunks):
    sky = lax.axis_index("sky")
    lane = lax.broadcasted_iota(jnp.int32, (SUB, LANES), 1)
    taps = trail_ref.shape[0]
    for p in range(trail_ref.shape[1]):
        for a in range(taps):
            for b in range(taps):
                value = jnp.zeros((SUB, LANES), jnp.float32) + trail_ref[a, p, b]
                trail_out[p, 0, a * taps + b] = value
                trail_out[p, 1, a * taps + b] = value * value
    stack_targets(outs, hops, wide, edge, offset_ref, shift_ref, sky, rows, chunks, lane)


def trail_kernel_body(trail_ref, *rest, rows, chunks, taps):
    parts = rest[:-2]
    out, image = rest[-2:]
    sky = lax.axis_index("sky")
    lane = lax.broadcasted_iota(jnp.int32, (SUB, LANES), 1)
    zero = jnp.zeros((SUB, LANES), jnp.float32)
    half = taps // 2
    groups = rows // SUB
    for p in range(out.shape[0]):
        def total(row, count):
            value = parts[0][p, row : row + count, :]
            for part in parts[1:]:
                value = value + part[p, row : row + count, :]
            return value

        results = []
        edges = total(2 * chunks * rows, 2 * chunks)
        for k in range(2):
            for c in range(chunks):
                image[c, 0:SUB, :] = zero
                image[c, SUB + rows :, :] = zero
                for g in range(groups):
                    image[c, SUB + g * SUB : SUB + (g + 1) * SUB, :] = total((k * chunks + c) * rows + g * SUB, SUB)
                at = jnp.where(sky == 0, SUB + rows, SUB - 1)
                image[c, pl.ds(at, 1), :] = edges[2 * c + k : 2 * c + k + 1, :]
            scale = [[trail_ref[p, k, a * taps + b] for b in range(taps)] for a in range(taps)]
            kind = []
            for g in range(groups):
                def load(a, c):
                    return image[c, SUB + g * SUB + a - half : SUB + g * SUB + a - half + SUB, :]

                kind.append(filter_rows(load, scale, taps, chunks, lane))
            results.append(kind)
        for g in range(groups):
            for c in range(chunks):
                value = results[0][g][c] / jnp.sqrt(results[1][g][c] + 1.0)
                out[p, g * SUB : (g + 1) * SUB, c * LANES : (c + 1) * LANES] = value


SMEM = pl.BlockSpec(memory_space=pltpu.SMEM)
VMEM = pl.BlockSpec(memory_space=pltpu.VMEM)
ANY = pl.BlockSpec(memory_space=pl.ANY)


def call(body, outputs, inputs, scratch=(), aliases={}, megabytes=8):
    return pl.pallas_call(
        body,
        out_shape=[jax.ShapeDtypeStruct(shape, jnp.float32) for shape in outputs],
        in_specs=[spec for spec, _ in inputs],
        out_specs=[VMEM] * len(outputs),
        scratch_shapes=scratch,
        input_output_aliases=aliases,
        compiler_params=pltpu.CompilerParams(vmem_limit_bytes=megabytes * 1024 * 1024),
    )(*[value for _, value in inputs])


def steps(
    science, inv_variance, pixel_masks, point_spread, tile_offset, column_shift, trail_kernel
):
    exposures, rows, width = science.shape
    chunks = width // LANES
    taps = point_spread.shape[-1]
    trail_taps = trail_kernel.shape[-1]
    count = lax.axis_size("expo")
    per = tile_offset.shape[0] // count

    weighted = inv_variance * pixel_masks.astype(jnp.float32)
    own = jnp.stack([science * weighted, weighted])
    other = lax.ppermute(own, "sky", [(0, 1), (1, 0)])

    spread = (SMEM, jnp.transpose(point_spread, (1, 0, 2)))
    offsets = (SMEM, tile_offset.T)
    shifts = (SMEM, column_shift.T)
    image_shape = (2, exposures, chunks, 2 * rows + 2 * SUB, LANES)
    wide_shape = (exposures, 2, chunks + 3, 2 * rows, LANES)
    edge_shape = (exposures, 2, chunks + 3, SUB, LANES)
    part = (per, 2 * chunks * rows + 2 * chunks, LANES)

    spread_shape = (exposures, 2, taps * taps, SUB, LANES)
    image, wide, spread = call(
        functools.partial(near_kernel, rows=rows, chunks=chunks, taps=taps),
        [image_shape, wide_shape, spread_shape], [spread, (VMEM, own)],
    )
    early, middle, late = stacking_order(count)
    results = call(
        functools.partial(far_kernel, hops=early, rows=rows, chunks=chunks, taps=taps),
        [image_shape, wide_shape, edge_shape] + [part] * len(early),
        [
            (VMEM, spread), (ANY, offsets[1]), (ANY, shifts[1]), (VMEM, other), (VMEM, image), (VMEM, wide),
        ],
        scratch=[
            pltpu.SMEM(offsets[1].shape, jnp.int32), pltpu.SMEM(shifts[1].shape, jnp.int32),
            pltpu.SemaphoreType.DMA(()), pltpu.SemaphoreType.DMA(()),
        ],
        aliases={4: 0, 5: 1},
    )
    wide, edge = results[1:3]
    parts = dict(zip(early, results[3:]))
    results = call(
        functools.partial(rest_kernel, hops=middle, rows=rows, chunks=chunks),
        [part] * len(middle), [offsets, shifts, (VMEM, wide), (VMEM, edge)],
    )
    parts.update(zip(middle, results))
    results = call(
        functools.partial(last_kernel, hops=late, rows=rows, chunks=chunks),
        [(per, 2, trail_taps * trail_taps, SUB, LANES)] + [part] * len(late),
        [offsets, shifts, (SMEM, jnp.transpose(trail_kernel, (1, 0, 2))), (VMEM, wide), (VMEM, edge)],
    )
    trail = results[0]
    parts.update(zip(late, results[1:]))

    bit = 1
    while bit < count:
        pairs = [
            (2 * i + core, 2 * (i ^ (turned(bit) if core else bit)) + core)
            for i in range(count) for core in range(2)
        ]
        for hop in range(count - bit, 0, -2 * bit):
            moved = lax.ppermute(parts[hop], ("expo", "sky"), pairs)
            parts[hop - bit] = parts[hop - bit] + moved
        bit *= 2
    total = parts[0]

    return call(
        functools.partial(trail_kernel_body, rows=rows, chunks=chunks, taps=trail_taps),
        [(per, rows, width)],
        [(VMEM, trail), (VMEM, total)],
        scratch=[pltpu.VMEM((chunks, rows + 2 * SUB, LANES), jnp.float32)],
    )[0]


def stacking_order(count):
    early = [hop for hop in (count - 1, count - 3) if hop > 0]
    middle = [hop for hop in (count - 2, count - 5) if hop > 0 and hop not in early]
    return early, middle, [hop for hop in range(count - 1, -1, -1) if hop not in early + middle]


def solution(mesh):
    return jax.shard_map(
        steps,
        mesh=mesh,
        in_specs=(
            P(("field", "expo"), "sky", None),
            P(("field", "expo"), "sky", None),
            P(("field", "expo"), "sky", None),
            P(("field", "expo"), None, None),
            P(None, "expo"),
            P(None, "expo"),
            P("expo", None, None),
        ),
        out_specs=P(("field", "expo"), "sky", None),
        check_vma=False,
    )
```

```python
import functools

import jax
import jax.numpy as jnp
from jax import lax
from jax.experimental import pallas as pl
from jax.experimental.pallas import tpu as pltpu
from jax.sharding import PartitionSpec as P


MAX_SHIFT = 128
LANES = 128
SUB = 8


def lane_shifted(pieces, lane, offset):
    if offset == 0:
        return pieces
    count = len(pieces)
    rolled = [pltpu.roll(piece, (-offset) % LANES, 1) for piece in pieces]
    out = []
    for c in range(count):
        near = rolled[c]
        if offset > 0:
            far = rolled[c + 1] if c + 1 < count else jnp.zeros_like(near)
            out.append(jnp.where(lane < LANES - offset, near, far))
        else:
            far = rolled[c - 1] if c > 0 else jnp.zeros_like(near)
            out.append(jnp.where(lane >= -offset, near, far))
    return out


def filter_rows(load, taps, row_taps, chunks, lane):
    half = row_taps // 2
    columns = [[None] * chunks for _ in range(row_taps)]
    for c in range(chunks):
        rows = [load(a, c) for a in range(row_taps)]
        for b in range(row_taps):
            total = rows[0] * taps[0][b]
            for a in range(1, row_taps):
                total = total + rows[a] * taps[a][b]
            columns[b][c] = total
    result = columns[half]
    for b in range(row_taps):
        if b != half:
            moved = lane_shifted(columns[b], lane, b - half)
            result = [x + y for x, y in zip(result, moved)]
    return result


def filter_groups(image, wide, taps_of, first, count, exposures, chunks, taps, lane):
    half = taps // 2
    for e in range(exposures):
        for k in range(2):
            scale = taps_of(e, k)
            for g in range(count):
                row = pl.multiple_of((first + g) * SUB, SUB)

                def load(a, c):
                    return image[k, e, c, pl.ds(row + (SUB + a - half), SUB), :]

                result = filter_rows(load, scale, taps, chunks, lane)
                for c in range(chunks):
                    wide[e, k, 1 + c, pl.ds(row, SUB), :] = result[c]


def taps_in(spread_ref, taps):
    def taps_of(e, k):
        scale = [[spread_ref[a, e, b] for b in range(taps)] for a in range(taps)]
        return scale if k == 0 else [[x * x for x in line] for line in scale]

    return taps_of


def vectors_in(load, taps):
    return lambda e, k: [[load(e, k, a * taps + b) for b in range(taps)] for a in range(taps)]


def near_kernel(spread_ref, own_ref, image, wide, spread_out, *, rows, chunks, taps):
    exposures = own_ref.shape[1]
    sky = lax.axis_index("sky")
    lane = lax.broadcasted_iota(jnp.int32, (SUB, LANES), 1)
    zero = jnp.zeros((SUB, LANES), jnp.float32)
    base = pl.multiple_of(SUB + rows * sky, SUB)
    for k in range(2):
        for e in range(exposures):
            for c in range(chunks):
                image[k, e, c, 0:SUB, :] = zero
                image[k, e, c, SUB + 2 * rows :, :] = zero
                image[k, e, c, pl.ds(base, rows), :] = own_ref[k, e, :, c * LANES : (c + 1) * LANES]
    inside = rows // SUB - 1
    first = (2 * (rows // SUB) - inside) * sky
    scalars = taps_in(spread_ref, taps)

    def taps_of(e, k):
        scale = [[zero + x for x in line] for line in scalars(e, k)]
        for a in range(taps):
            for b in range(taps):
                spread_out[e, k, a * taps + b] = scale[a][b]
        return scale

    filter_groups(image, wide, taps_of, first, inside, exposures, chunks, taps, lane)
    blank = jnp.zeros((2 * rows, LANES), jnp.float32)
    for e in range(exposures):
        for k in range(2):
            for c in (0, chunks + 1, chunks + 2):
                wide[e, k, c] = blank


def stack_velocity(out, p, v, wide, edge, offset_ref, shift_ref, sky, rows, chunks, lane):
    exposures = wide.shape[0]
    totals = [None, None]
    edges = None
    groups = rows // SUB
    for e in range(exposures):
        tile = lax.rem(sky + offset_ref[e, v], 2)
        start = MAX_SHIFT - shift_ref[e, v]
        skip = lax.div(start, LANES)
        turn = lax.rem(start, LANES)
        back = lax.rem(LANES - turn, LANES)
        keep = lane < LANES - turn
        base = pl.multiple_of(tile * rows, SUB)
        for k in range(2):
            moved = [
                [
                    pltpu.roll(wide[e, k, skip + c, pl.ds(pl.multiple_of(base + g * SUB, SUB), SUB), :], back, 1)
                    for g in range(groups)
                ]
                for c in range(chunks + 1)
            ]
            picked = [
                [jnp.where(keep, moved[c][g], moved[c + 1][g]) for g in range(groups)] for c in range(chunks)
            ]
            if totals[k] is None:
                totals[k] = picked
            else:
                totals[k] = [[x + y for x, y in zip(p0, p1)] for p0, p1 in zip(totals[k], picked)]
        moved = [pltpu.roll(edge[e, 1 - tile, skip + c], back, 1) for c in range(chunks + 1)]
        picked = [jnp.where(keep, moved[c], moved[c + 1]) for c in range(chunks)]
        edges = picked if edges is None else [x + y for x, y in zip(edges, picked)]
    for k in range(2):
        for c in range(chunks):
            for g in range(groups):
                row = (k * chunks + c) * rows + g * SUB
                out[p, row : row + SUB, :] = totals[k][c][g]
    for c in range(chunks):
        row = 2 * chunks * rows + 2 * c
        out[p, row : row + 2, :] = edges[c][0:2, :]


def stack_targets(outs, hops, wide, edge, offset_ref, shift_ref, sky, rows, chunks, lane):
    me = lax.axis_index("expo")
    for out, hop in zip(outs, hops):
        owner = jnp.bitwise_xor(me, jnp.where(sky == 0, hop, turned(hop)))
        for p in range(out.shape[0]):
            stack_velocity(
                out, p, owner * out.shape[0] + p, wide, edge, offset_ref, shift_ref, sky, rows, chunks, lane
            )


def turned(hop):
    return (hop & ~3) | ((hop & 1) << 1) | ((hop >> 1) & 1)


def far_kernel(
    spread_ref, offset_from, shift_from, other_ref, image_in, wide_in, image, wide, edge, *rest,
    hops, rows, chunks, taps,
):
    outs = rest[: len(hops)]
    offset_ref, shift_ref, offset_sem, shift_sem = rest[len(hops):]
    offset_copy = pltpu.make_async_copy(offset_from, offset_ref, offset_sem)
    shift_copy = pltpu.make_async_copy(shift_from, shift_ref, shift_sem)
    offset_copy.start()
    shift_copy.start()
    exposures = other_ref.shape[1]
    sky = lax.axis_index("sky")
    lane = lax.broadcasted_iota(jnp.int32, (SUB, LANES), 1)
    zero = jnp.zeros((SUB, LANES), jnp.float32)
    base = pl.multiple_of(SUB + rows * (1 - sky), SUB)
    for k in range(2):
        for e in range(exposures):
            for c in range(chunks):
                image[k, e, c, pl.ds(base, rows), :] = other_ref[k, e, :, c * LANES : (c + 1) * LANES]
    inside = rows // SUB - 1
    filter_groups(
        image, wide, vectors_in(lambda e, k, i: spread_ref[e, k, i], taps), inside * (1 - sky),
        2 * (rows // SUB) - inside, exposures, chunks, taps, lane,
    )
    at_row = (rows - 1) * sky
    for e in range(exposures):
        for t in range(2):
            for c in (0, chunks + 1, chunks + 2):
                edge[e, t, c] = zero
            for k in range(2):
                for c in range(chunks):
                    edge[e, t, 1 + c, k : k + 1, :] = wide[e, k, 1 + c, pl.ds(rows * t + at_row, 1), :]
    offset_copy.wait()
    shift_copy.wait()
    stack_targets(outs, hops, wide, edge, offset_ref, shift_ref, sky, rows, chunks, lane)


def rest_kernel(offset_ref, shift_ref, trail_ref, wide, edge, trail_out, *outs, hops, rows, chunks):
    sky = lax.axis_index("sky")
    lane = lax.broadcasted_iota(jnp.int32, (SUB, LANES), 1)
    taps = trail_ref.shape[0]
    for p in range(trail_ref.shape[1]):
        for a in range(taps):
            for b in range(taps):
                value = jnp.zeros((SUB, LANES), jnp.float32) + trail_ref[a, p, b]
                trail_out[p, 0, a * taps + b] = value
                trail_out[p, 1, a * taps + b] = value * value
    stack_targets(outs, hops, wide, edge, offset_ref, shift_ref, sky, rows, chunks, lane)


def trail_kernel_body(trail_ref, *rest, rows, chunks, taps):
    parts = rest[:-2]
    out, image = rest[-2:]
    sky = lax.axis_index("sky")
    lane = lax.broadcasted_iota(jnp.int32, (SUB, LANES), 1)
    zero = jnp.zeros((SUB, LANES), jnp.float32)
    half = taps // 2
    groups = rows // SUB
    for p in range(out.shape[0]):
        def total(row, count):
            value = parts[0][p, row : row + count, :]
            for part in parts[1:]:
                value = value + part[p, row : row + count, :]
            return value

        results = []
        edges = total(2 * chunks * rows, 2 * chunks)
        for k in range(2):
            for c in range(chunks):
                image[c, 0:SUB, :] = zero
                image[c, SUB + rows :, :] = zero
                for g in range(groups):
                    image[c, SUB + g * SUB : SUB + (g + 1) * SUB, :] = total((k * chunks + c) * rows + g * SUB, SUB)
                at = jnp.where(sky == 0, SUB + rows, SUB - 1)
                image[c, pl.ds(at, 1), :] = edges[2 * c + k : 2 * c + k + 1, :]
            scale = [[trail_ref[p, k, a * taps + b] for b in range(taps)] for a in range(taps)]
            kind = []
            for g in range(groups):
                def load(a, c):
                    return image[c, SUB + g * SUB + a - half : SUB + g * SUB + a - half + SUB, :]

                kind.append(filter_rows(load, scale, taps, chunks, lane))
            results.append(kind)
        for g in range(groups):
            for c in range(chunks):
                value = results[0][g][c] / jnp.sqrt(results[1][g][c] + 1.0)
                out[p, g * SUB : (g + 1) * SUB, c * LANES : (c + 1) * LANES] = value


SMEM = pl.BlockSpec(memory_space=pltpu.SMEM)
VMEM = pl.BlockSpec(memory_space=pltpu.VMEM)
ANY = pl.BlockSpec(memory_space=pl.ANY)


def call(body, outputs, inputs, scratch=(), aliases={}, megabytes=8):
    return pl.pallas_call(
        body,
        out_shape=[jax.ShapeDtypeStruct(shape, jnp.float32) for shape in outputs],
        in_specs=[spec for spec, _ in inputs],
        out_specs=[VMEM] * len(outputs),
        scratch_shapes=scratch,
        input_output_aliases=aliases,
        compiler_params=pltpu.CompilerParams(vmem_limit_bytes=megabytes * 1024 * 1024),
    )(*[value for _, value in inputs])


def steps(
    science, inv_variance, pixel_masks, point_spread, tile_offset, column_shift, trail_kernel
):
    exposures, rows, width = science.shape
    chunks = width // LANES
    taps = point_spread.shape[-1]
    trail_taps = trail_kernel.shape[-1]
    count = lax.axis_size("expo")
    per = tile_offset.shape[0] // count

    weighted = inv_variance * pixel_masks.astype(jnp.float32)
    own = jnp.stack([science * weighted, weighted])
    other = lax.ppermute(own, "sky", [(0, 1), (1, 0)])

    spread = (SMEM, jnp.transpose(point_spread, (1, 0, 2)))
    offsets = (SMEM, tile_offset.T)
    shifts = (SMEM, column_shift.T)
    image_shape = (2, exposures, chunks, 2 * rows + 2 * SUB, LANES)
    wide_shape = (exposures, 2, chunks + 3, 2 * rows, LANES)
    edge_shape = (exposures, 2, chunks + 3, SUB, LANES)
    part = (per, 2 * chunks * rows + 2 * chunks, LANES)

    spread_shape = (exposures, 2, taps * taps, SUB, LANES)
    image, wide, spread = call(
        functools.partial(near_kernel, rows=rows, chunks=chunks, taps=taps),
        [image_shape, wide_shape, spread_shape], [spread, (VMEM, own)],
    )
    early, late = sending_order(count)
    results = call(
        functools.partial(far_kernel, hops=early, rows=rows, chunks=chunks, taps=taps),
        [image_shape, wide_shape, edge_shape] + [part] * len(early),
        [
            (VMEM, spread), (ANY, offsets[1]), (ANY, shifts[1]), (VMEM, other), (VMEM, image), (VMEM, wide),
        ],
        scratch=[
            pltpu.SMEM(offsets[1].shape, jnp.int32), pltpu.SMEM(shifts[1].shape, jnp.int32),
            pltpu.SemaphoreType.DMA(()), pltpu.SemaphoreType.DMA(()),
        ],
        aliases={4: 0, 5: 1},
    )
    wide, edge = results[1:3]
    parts = dict(zip(early, results[3:]))
    results = call(
        functools.partial(rest_kernel, hops=late, rows=rows, chunks=chunks),
        [(per, 2, trail_taps * trail_taps, SUB, LANES)] + [part] * len(late),
        [offsets, shifts, (SMEM, jnp.transpose(trail_kernel, (1, 0, 2))), (VMEM, wide), (VMEM, edge)],
    )
    trail = results[0]
    parts.update(zip(late, results[1:]))

    bit = 1
    while bit < count:
        pairs = [
            (2 * i + core, 2 * (i ^ (turned(bit) if core else bit)) + core)
            for i in range(count) for core in range(2)
        ]
        for hop in range(count - bit, 0, -2 * bit):
            moved = lax.ppermute(parts[hop], ("expo", "sky"), pairs)
            parts[hop - bit] = parts[hop - bit] + moved
        bit *= 2
    total = parts[0]

    return call(
        functools.partial(trail_kernel_body, rows=rows, chunks=chunks, taps=trail_taps),
        [(per, rows, width)],
        [(VMEM, trail), (VMEM, total)],
        scratch=[pltpu.VMEM((chunks, rows + 2 * SUB, LANES), jnp.float32)],
    )[0]


def sending_order(count):
    hops = list(range(count - 1, 0, -2)) + list(range(count - 2, -1, -2))
    early = [hop for hop in (count - 1, count // 2 - 1) if hop > 0]
    return early, [hop for hop in hops if hop not in early]


def solution(mesh):
    return jax.shard_map(
        steps,
        mesh=mesh,
        in_specs=(
            P(("field", "expo"), "sky", None),
            P(("field", "expo"), "sky", None),
            P(("field", "expo"), "sky", None),
            P(("field", "expo"), None, None),
            P(None, "expo"),
            P(None, "expo"),
            P("expo", None, None),
        ),
        out_specs=P(("field", "expo"), "sky", None),
        check_vma=False,
    )
```
